256 devices in a mesh: seq: 128 (over z, x, y), dp: 2 (over core).
Axes of the slice: x: 4, y: 4, z: 8, core: 2. Of those that a mesh axis runs over, the one named last changes fastest.
Arguments:
- queries: bfloat16 [2, 24576, 4096], P('dp', 'seq'), may hold values from -6 to 6
- key_vectors: bfloat16 [2, 24576, 4096], P('dp', 'seq'), may hold values from -0.52734375 to 0.52734375
- value_vectors: bfloat16 [2, 24576, 4096], P('dp', 'seq'), may hold values from -6 to 6
- out_grad: bfloat16 [2, 24576, 4096], P('dp', 'seq'), may hold values from -24 to 24
- log_decay: float32 [2, 32, 24576], P('dp', None, 'seq'), may hold values from -0.7729167 to 0, as said below
- norm_gain: float32 [4096], replicated, may hold values from 0.25 to 1.75
Outputs:
- output: bfloat16 [2, 24576, 4096], P('dp', 'seq')
- grad_queries: bfloat16 [2, 24576, 4096], P('dp', 'seq')
- grad_keys: bfloat16 [2, 24576, 4096], P('dp', 'seq')
- grad_values: bfloat16 [2, 24576, 4096], P('dp', 'seq')
- grad_gain: float32 [4096], P('seq')
The draws below stay inside these ranges and needn't reach their ends.
Inputs may be any that keep to these rules, and one draw needn't show every extreme that they name: `log_decay`: every entry is negative.
All inputs are finite; a program needn't handle non-finite values.
Results may differ from the reference program's by a relative error of at most 0.006.
Values may be sent and summed in bfloat16 or wider, within the bound.
A program may use at most 128 MiB of HBM per device.

```python
import math
import jax
import jax.numpy as jnp
from jax import lax

HEADS = 32
HEAD_DIM = 128
TOK_DEV = 192
SEQUENCE_LENGTH = 24576
SEQS = 2


def draw_log_decay(key, part):
    head_random_key, quick_random_key, gradual_random_key, noise_random_key, spike_random_key, dropout_random_key = jax.random.split(key, 6)
    chosen = jax.random.uniform(head_random_key, (HEADS,))
    is_fast = chosen < 0.5
    fast_rate = jnp.exp(jax.random.uniform(quick_random_key, (HEADS,), minval=math.log(4.0 / TOK_DEV), maxval=math.log(7.0 / TOK_DEV)))
    slow_rate = jnp.exp(jax.random.uniform(gradual_random_key, (HEADS,), minval=math.log(0.1 / SEQUENCE_LENGTH), maxval=math.log(0.5 / SEQUENCE_LENGTH)))
    baseline_decay_rate = jnp.where(is_fast, fast_rate, slow_rate)
    sharding_arrangement = (SEQS, HEADS, SEQUENCE_LENGTH)
    decay_noise = jnp.exp(jax.random.uniform(noise_random_key, sharding_arrangement, minval=-0.69, maxval=0.69))
    decay_spikes = jax.random.uniform(spike_random_key, sharding_arrangement) < 2.0 / SEQUENCE_LENGTH
    dropped_log_decay = jax.random.uniform(dropout_random_key, sharding_arrangement, minval=-0.69, maxval=-0.22)
    return (-baseline_decay_rate[None, :, None] * decay_noise + jnp.where(decay_spikes, dropped_log_decay, 0.0)).astype(jnp.float32)


def spiked(entries, own_key, source, target, parts, factor):
    def block_of(dim):
        return (jnp.arange(entries.shape[dim]) // (entries.shape[dim] // parts)).reshape((-1,) + (1,) * (entries.ndim - 1 - dim))

    near = jax.random.permutation(own_key, parts)[block_of(target)]
    other_side = (block_of(target) + parts // 2) % parts
    return jnp.where((block_of(source) == near) | (block_of(source) == other_side), factor * entries, entries)


def level_of(key, extent, shards, low, largest):
    factor_of, own = 1.0, jax.random.fold_in(key, 6)
    for position, shards_of in shards:
        heights = jnp.exp(jax.random.uniform(jax.random.fold_in(own, position), (shards_of,), jnp.float32, low / len(shards), largest / len(shards)))
        factor_of = factor_of * jnp.repeat(heights, extent[position] // shards_of).reshape([-1 if axis == position else 1 for axis in range(len(extent))])
    return factor_of


def noise(key, extent, deviation, bound, pieces=(), kind=jnp.bfloat16):
    gain = level_of(key, extent, pieces, -0.22, 0.18) if pieces else 1.0
    drawn = jax.random.normal(key, extent, jnp.float32) * deviation * gain
    return jnp.minimum(jnp.maximum(drawn, -bound), bound).astype(kind)


def heavy_noise(rng, dims, width, most, cuts, heavy, held_as=jnp.bfloat16):
    drawn = width * jax.random.normal(rng, dims, jnp.float32)
    if cuts:
        drawn = drawn * level_of(rng, dims, cuts, -0.22, 0.18)
    return jnp.clip(spiked(drawn, jax.random.fold_in(rng, 3), *heavy), -most, most).astype(held_as)


def setup_inputs(seed: int = 0) -> dict:
    splits = jax.random.split(jax.random.key(seed), 7)
    queries = noise(splits[0], (SEQS, SEQUENCE_LENGTH, HEADS * HEAD_DIM), 1.0, 6.0, ((0, 2), (1, 128)))
    key_vectors = noise(splits[1], (SEQS, SEQUENCE_LENGTH, HEADS * HEAD_DIM), (HEAD_DIM ** -0.5), 0.52734375, ((0, 2), (1, 128)))
    value_vectors = noise(splits[2], (SEQS, SEQUENCE_LENGTH, HEADS * HEAD_DIM), 1.0, 6.0, ((0, 2), (1, 128)))
    out_grad = heavy_noise(splits[3], (SEQS, SEQUENCE_LENGTH, HEADS * HEAD_DIM), 1.0, 24.0, ((0, 2), (1, 128)), (1, 2, 128, 5.5))
    log_decay = draw_log_decay(jax.random.fold_in(splits[6], 71), 0)
    norm_gain = jnp.clip(1.0 + 0.15 * jax.random.normal(splits[5], (HEADS * HEAD_DIM,), jnp.float32), 0.25, 1.75)
    return {"queries": queries, "key_vectors": key_vectors, "value_vectors": value_vectors, "out_grad": out_grad, "log_decay": log_decay, "norm_gain": norm_gain}


epsilon = 1e-06

def widen(array):
    return array.astype(jnp.float32)

def decays(cumul, block_total, block_len):
    positions = jnp.arange(block_len)
    causal = (positions[:, None] >= positions[None, :])[None]
    log_gap = cumul[:, :, None] - cumul[:, None, :]
    weight = jnp.where(causal, jnp.exp(jnp.where(causal, log_gap, 0.0)), 0.0)
    start_scale = jnp.exp(cumul).T[:, :, None]
    end_scale = jnp.exp(block_total[:, None] - cumul).T[:, :, None]
    return (weight, start_scale, end_scale)

def single_sequence(inputs):
    query_seq, key_seq, value_seq, grad_seq, decay_seq, norm_gain = inputs
    length, feature_count = query_seq.shape
    head_count = decay_seq.shape[0]
    head_size = feature_count // head_count
    block_len = TOK_DEV
    block_count = length // block_len
    sequence_partition = (block_count, block_len, head_count, head_size)
    query_blocks = query_seq.reshape(sequence_partition)
    key_blocks = key_seq.reshape(sequence_partition)
    value_blocks = value_seq.reshape(sequence_partition)
    decay_blocks = decay_seq.reshape(head_count, block_count, block_len).transpose(1, 0, 2)
    cumulative = jnp.cumsum(decay_blocks, axis=2)
    totals = cumulative[:, :, -1]

    def forward_step(state, inputs_now):
        query_now, key_now, value_now, cumul, block_total = inputs_now
        weight, start_scale, end_scale = decays(cumul, block_total, block_len)
        scores = jnp.einsum('ihe,jhe->hij', widen(query_now), widen(key_now))
        weighted = (scores * weight).astype(jnp.bfloat16)
        inside = jnp.einsum('hij,jhe->ihe', widen(weighted), widen(value_now))
        prior_state = state.astype(jnp.bfloat16)
        carried = jnp.einsum('ihd,hde->ihe', widen(query_now), widen(prior_state)) * start_scale
        key_decayed = (widen(key_now) * end_scale).astype(jnp.bfloat16)
        local_state = jnp.einsum('jhd,jhe->hde', widen(key_decayed), widen(value_now))
        next_state = jnp.exp(block_total)[:, None, None] * state + local_state
        return (next_state, (inside + carried, prior_state))
    start = jnp.zeros((head_count, head_size, head_size), jnp.float32)
    unused, (attended, priors) = lax.scan(forward_step, start, (query_blocks, key_blocks, value_blocks, cumulative, totals))
    inv_rms = lax.rsqrt(lax.optimization_barrier(jnp.mean(attended * attended, axis=-1, keepdims=True)) + epsilon)
    normed = attended * inv_rms
    gain_heads = norm_gain.reshape(head_count, head_size)
    output = (normed * gain_heads).astype(jnp.bfloat16)
    grad_out = widen(grad_seq.reshape(sequence_partition))
    scaled = grad_out * gain_heads
    grad_attended = (inv_rms * (scaled - normed * lax.optimization_barrier(jnp.mean(scaled * normed, axis=-1, keepdims=True)))).astype(jnp.bfloat16)
    gain_term = lax.optimization_barrier(jnp.sum(grad_out * normed, axis=(0, 1))).reshape(feature_count)

    def backward_step(later, inputs_now):
        query_now, key_now, value_now, grad_now, cumul, block_total, prior_state = inputs_now
        weight, start_scale, end_scale = decays(cumul, block_total, block_len)
        scores = jnp.einsum('ihe,jhe->hij', widen(query_now), widen(key_now))
        weighted = (scores * weight).astype(jnp.bfloat16)
        later_state = later.astype(jnp.bfloat16)
        grad_scores = jnp.einsum('ihe,jhe->hij', widen(grad_now), widen(value_now))
        grad_weighted = (grad_scores * weight).astype(jnp.bfloat16)
        grad_query = jnp.einsum('hij,jhd->ihd', widen(grad_weighted), widen(key_now)) + start_scale * jnp.einsum('ihe,hde->ihd', widen(grad_now), widen(prior_state))
        grad_key = jnp.einsum('hij,ihd->jhd', widen(grad_weighted), widen(query_now)) + end_scale * jnp.einsum('jhe,hde->jhd', widen(value_now), widen(later_state))
        grad_value = jnp.einsum('hij,ihe->jhe', widen(weighted), widen(grad_now)) + end_scale * jnp.einsum('jhd,hde->jhe', widen(key_now), widen(later_state))
        query_decayed = (widen(query_now) * start_scale).astype(jnp.bfloat16)
        later_local = jnp.einsum('ihd,ihe->hde', widen(query_decayed), widen(grad_now))
        next_later = later_local + jnp.exp(block_total)[:, None, None] * later
        return (next_later, (grad_query.astype(jnp.bfloat16), grad_key.astype(jnp.bfloat16), grad_value.astype(jnp.bfloat16)))
    unused_later, grads = lax.scan(backward_step, start, (query_blocks, key_blocks, value_blocks, grad_attended, cumulative, totals, priors), reverse=True)
    shape_out = (length, feature_count)
    return (output.reshape(shape_out), grads[0].reshape(shape_out), grads[1].reshape(shape_out), grads[2].reshape(shape_out), gain_term)

def reference(queries, key_vectors, value_vectors, out_grad, log_decay, norm_gain):
    seq_count = queries.shape[0]
    gains = jnp.broadcast_to(norm_gain, (seq_count,) + norm_gain.shape)
    results = lax.map(single_sequence, (queries, key_vectors, value_vectors, out_grad, log_decay, gains))
    return (results[0], results[1], results[2], results[3], lax.optimization_barrier(jnp.sum(results[4], axis=0)))
```

```python
import functools

import jax
import jax.numpy as jnp
from jax import lax
from jax.experimental import pallas as pl
from jax.experimental.pallas import tpu as pltpu
from jax.sharding import Mesh
from jax.sharding import PartitionSpec as P

AXES = ("z", "x", "y", "dp")
SEQ = ("z", "x", "y")
SIZES = {"z": 8, "x": 4, "y": 4, "dp": 2}
NZ, NX, NY = 8, 4, 4
D = 128
OWN = 8
G = 4
HPG = OWN // G
R = HPG * D
RX = R // NX
BF = jnp.bfloat16
F32 = jnp.float32
epsilon = 1e-06


def here():
    return {name: lax.axis_index(name) for name in AXES}


def shifted(me, axis, step):
    there = dict(me)
    there[axis] = lax.rem(me[axis] + step, SIZES[axis])
    return tuple(there[name] for name in AXES)


def push(src, dst, send, recv, target):
    return pltpu.make_async_remote_copy(
        src_ref=src,
        dst_ref=dst,
        send_sem=send,
        recv_sem=recv,
        device_id=target,
        device_id_type=pl.DeviceIdType.MESH,
    )


class Wire:
    def __init__(self, me, axis, sems):
        self.me, self.axis, self.sems = me, axis, sems
        self.steps = range(1, SIZES[axis])
        self.open = []

    def peer(self, step):
        return lax.rem(self.me[self.axis] + step, SIZES[self.axis])

    def send(self, step, key, src, dst):
        send, recv = self.sems
        copy = push(src, dst, send.at[step - 1, key], recv.at[step - 1, key], shifted(self.me, self.axis, step))
        copy.start()
        self.open.append(copy)

    def arrived(self, step, key, dst):
        send, recv = self.sems
        push(dst, dst, send.at[step - 1, key], recv.at[step - 1, key], shifted(self.me, self.axis, step)).wait_recv()

    def drain(self):
        for copy in self.open:
            copy.wait_send()


def sem_pair(axis, keys):
    return [pltpu.SemaphoreType.DMA((SIZES[axis] - 1, keys))] * 2


def slot_of(me, axis, index):
    n = SIZES[axis]
    return lax.rem(me[axis] + (n - 1) + (n - index), n)


def greet(me):
    barrier = pltpu.get_barrier_semaphore()
    count = 0
    for axis in AXES:
        for step in range(1, SIZES[axis]):
            pl.semaphore_signal(
                barrier, inc=1, device_id=shifted(me, axis, step), device_id_type=pl.DeviceIdType.MESH
            )
            count += 1
    return lambda: pl.semaphore_wait(barrier, count)


class Decays:
    scratch = [
        pltpu.VMEM((NY, OWN, D), F32),
        pltpu.VMEM((NX, OWN, D), F32),
        pltpu.VMEM((NZ, OWN, D), F32),
        *sem_pair("y", 1),
        *sem_pair("x", 1),
        *sem_pair("z", 1),
    ]

    def __init__(self, me, refs, total):
        self.me, self.total = me, total
        self.levels = dict(zip("yxz", refs[:3]))
        self.wires = {a: Wire(me, a, refs[3 + 2 * i : 5 + 2 * i]) for i, a in enumerate("yxz")}

    def start(self):
        level, wire = self.levels["y"], self.wires["y"]
        for step in wire.steps:
            wire.send(step, 0, self.total.at[wire.peer(step)], level.at[step - 1])
        level[NY - 1] = self.total[self.me["y"]]

    def settle(self, axis):
        for step in self.wires[axis].steps:
            self.wires[axis].arrived(step, 0, self.levels[axis].at[step - 1])

    def lift(self, low, high):
        self.settle(low)
        n, m = SIZES[low], SIZES[high]
        level, above, wire = self.levels[low], self.levels[high], self.wires[high]
        above[m - 1] = functools.reduce(jnp.add, [level[slot_of(self.me, low, k)] for k in range(n)])
        for step in wire.steps:
            wire.send(step, 0, above.at[m - 1], above.at[step - 1])

    def row(self, axis, slot, head):
        return jnp.exp(self.levels[axis][slot, pl.ds(head, 1), :])

    def drain(self):
        for wire in self.wires.values():
            wire.drain()


class Scan:
    scratch = [
        pltpu.VMEM((NY, G, R, D), BF),
        pltpu.VMEM((NX, G, RX, D), BF),
        pltpu.VMEM((NX, G, RX, D), BF),
        pltpu.VMEM((NZ, G, RX, D), BF),
        pltpu.VMEM((NX, G, RX, D), BF),
        pltpu.VMEM((G, NX, RX, D), BF),
        pltpu.VMEM((NY, G, R, D), BF),
        *sem_pair("y", G),
        *sem_pair("x", G),
        *sem_pair("z", G),
        *sem_pair("x", G),
        *sem_pair("y", G),
    ]

    def __init__(self, me, refs, decays, prior, backward):
        self.me, self.decays, self.prior, self.backward = me, decays, prior, backward
        self.yin, self.xin, self.xout, self.zin, self.lines, self.line, self.yout = refs[:7]
        sems = refs[7:]
        names = ("y", "x", "z", "x", "y")
        self.y, self.x, self.z, self.xback, self.yback = [
            Wire(me, a, sems[2 * i : 2 * i + 2]) for i, a in enumerate(names)
        ]

    def order(self, n):
        return list(range(n))[:: -1 if self.backward else 1]

    def start(self, g, source):
        for step in self.y.steps:
            self.y.send(step, g, source(self.y.peer(step)), self.yin.at[step - 1, g])

    def over_lines(self, g):
        me = self.me
        for step in self.y.steps:
            self.y.arrived(step, g, self.yin.at[step - 1, g])
        for i in range(HPG):
            rows = pl.ds(i * D, D)
            total = None
            for k in self.order(NY):
                slot = slot_of(me, "y", k)
                term = self.yin[slot, g, rows, :].astype(F32)
                total = term if total is None else total * self.decays.row("y", slot, g * HPG + i) + term
            total = total.astype(BF)
            if RX >= D:
                per = RX // D
                self.xout[i // per, g, pl.ds((i % per) * D, D), :] = total
            else:
                per = D // RX
                for j in range(per):
                    self.xout[i * per + j, g] = total[j * RX : (j + 1) * RX]
        for step in self.x.steps:
            self.x.send(step, g, self.xout.at[self.x.peer(step), g], self.xin.at[step - 1, g])
        self.xin[NX - 1, g] = self.xout[me["x"], g]

    def pieces(self, g):
        first = g * HPG + (self.me["x"] * RX) // D
        return [(first + i, pl.ds(i * D, min(D, RX))) for i in range(max(1, RX // D))]

    def over_planes(self, g):
        me = self.me
        for step in self.x.steps:
            self.x.arrived(step, g, self.xin.at[step - 1, g])
        for head, rows in self.pieces(g):
            total = None
            for k in self.order(NX):
                slot = slot_of(me, "x", k)
                term = self.xin[slot, g, rows, :].astype(F32)
                total = term if total is None else total * self.decays.row("x", slot, head) + term
            self.zin[NZ - 1, g, rows, :] = total.astype(BF)
        for step in self.z.steps:
            self.z.send(step, g, self.zin.at[NZ - 1, g], self.zin.at[step - 1, g])

    def before_lines(self, g):
        me = self.me
        for step in self.z.steps:
            self.z.arrived(step, g, self.zin.at[step - 1, g])
        for head, rows in self.pieces(g):
            state = jnp.zeros((min(D, RX), D), F32)
            for k in self.order(NZ):
                slot = slot_of(me, "z", k)
                passed = (k > me["z"]) if self.backward else (k < me["z"])
                ahead = state * self.decays.row("z", slot, head) + self.zin[slot, g, rows, :].astype(F32)
                state = jnp.where(passed, ahead, state)
            for n, k in enumerate(self.order(NX)):
                self.lines[k, g, rows, :] = state.astype(BF)
                if n < NX - 1:
                    slot = slot_of(me, "x", k)
                    state = state * self.decays.row("x", slot, head) + self.xin[slot, g, rows, :].astype(F32)
        for step in self.xback.steps:
            self.xback.send(step, g, self.lines.at[self.xback.peer(step), g], self.line.at[g, me["x"]])
        self.line[g, me["x"]] = self.lines[me["x"], g]

    def before_blocks(self, g):
        me = self.me
        for step in self.xback.steps:
            self.xback.arrived(step, g, self.line.at[g, lax.rem(me["x"] + (NX - step), NX)])
        for i in range(HPG):
            rows = pl.ds(i * D, D)
            if RX >= D:
                per = RX // D
                state = self.line[g, i // per, pl.ds((i % per) * D, D), :].astype(F32)
            else:
                per = D // RX
                state = jnp.concatenate([self.line[g, i * per + j].astype(F32) for j in range(per)], axis=0)
            for n, k in enumerate(self.order(NY)):
                self.yout[k, g, rows, :] = state.astype(BF)
                if n < NY - 1:
                    slot = slot_of(me, "y", k)
                    row = self.decays.row("y", slot, g * HPG + i)
                    state = state * row + self.yin[slot, g, rows, :].astype(F32)
        for step in self.yback.steps:
            self.yback.send(step, g, self.yout.at[self.yback.peer(step), g], self.prior.at[me["y"], g])
        self.prior[me["y"], g] = self.yout[me["y"], g]

    def arrive(self, g, step):
        self.yback.arrived(step, g, self.prior.at[lax.rem(self.me["y"] + (NY - step), NY), g])

    def drain(self):
        for wire in (self.y, self.x, self.z, self.xback, self.yback):
            wire.drain()


class Gain:
    scratch = [
        pltpu.VMEM((NZ, 4, 8, D), F32),
        pltpu.VMEM((4, 8, D), F32),
        pltpu.VMEM((NX, 8, D), F32),
        pltpu.VMEM((NY, 8, D), F32),
        pltpu.VMEM((2, 8, D), F32),
        *sem_pair("z", 1),
        *sem_pair("x", 1),
        *sem_pair("y", 1),
        *sem_pair("dp", 1),
    ]

    def __init__(self, me, refs, part, out):
        self.me, self.part, self.out = me, part, out
        self.zin, self.plane, self.xin, self.yin, self.din = refs[:5]
        sems = refs[5:]
        self.z, self.x, self.y, self.dp = [
            Wire(me, a, sems[2 * i : 2 * i + 2]) for i, a in enumerate(("z", "x", "y", "dp"))
        ]

    def start(self):
        for step in self.z.steps:
            self.z.send(step, 0, self.part.at[pl.ds(4 * self.z.peer(step), 4)], self.zin.at[step - 1])
        self.zin[NZ - 1] = self.part[pl.ds(4 * self.me["z"], 4)]

    def total(self, wire, buffer):
        n = SIZES[wire.axis]
        for step in wire.steps:
            wire.arrived(step, 0, buffer.at[step - 1])
        return functools.reduce(jnp.add, [buffer[slot_of(self.me, wire.axis, k)] for k in range(n)])

    def over_z(self):
        self.plane[...] = self.total(self.z, self.zin)
        for step in self.x.steps:
            self.x.send(step, 0, self.plane.at[self.x.peer(step)], self.xin.at[step - 1])
        self.xin[NX - 1] = self.plane[self.me["x"]]

    def over_x(self):
        self.yin[NY - 1] = self.total(self.x, self.xin)
        for step in self.y.steps:
            self.y.send(step, 0, self.yin.at[NY - 1], self.yin.at[step - 1])

    def over_y(self):
        self.din[1] = self.total(self.y, self.yin)
        self.dp.send(1, 0, self.din.at[1], self.din.at[0])

    def over_dp(self):
        row = jnp.sum(self.total(self.dp, self.din), axis=0, keepdims=True)
        width = D // NY
        self.out[...] = functools.reduce(
            jnp.add,
            [
                jnp.where(self.me["y"] == k, row[:, k * width : (k + 1) * width], 0.0)
                for k in range(NY)
            ],
        )

    def drain(self):
        for wire in (self.z, self.x, self.y, self.dp):
            wire.drain()


T = 192
HEADS = NY * OWN

CHAIN = (
    ("local", 1.0, "y", 2.9),
    ("lines", 0.35, "x", 2.7),
    ("planes", 0.15, "z", 4.0),
    ("before_lines", 0.25, "x", 2.7),
    ("before_blocks", 0.5, "y", 2.9),
    ("middle", 2.2, "y", 2.9),
    ("back_lines", 0.35, "x", 2.7),
    ("back_planes", 0.15, "z", 4.0),
    ("back_before_lines", 0.25, "x", 2.7),
    ("back_before_blocks", 0.5, "y", 2.9),
    ("last", 1.5, None, 0.0),
)
BUSY = {"y": 11.5 / G, "x": 2.9 / G, "z": 11.5 / G}
FILL = (("early", "middle", 1.8), ("late", "last", 1.8))


def plan():
    rest = [sum(c[1] + c[3] for c in CHAIN[i:]) for i in range(len(CHAIN))]
    step_of = {c[0]: i for i, c in enumerate(CHAIN)}
    now, at, ready = 0.0, [0] * G, [0.0] * G
    links = {"y": 0.0, "x": 0.0, "z": 0.0}
    filled, order = set(), []
    after = {"early": -1, "late": step_of["middle"]}
    while any(a < len(CHAIN) for a in at):
        fits = []
        for g in range(G):
            if at[g] == len(CHAIN):
                continue
            name = CHAIN[at[g]][0]
            if ready[g] <= now:
                lacking = [f for f, s, _ in FILL if s == name and (f, g) not in filled]
                fits.append((-rest[at[g]], g, lacking[0] if lacking else name))
        if fits:
            _, g, name = min(fits)
        else:
            spare = [
                (g, f) for f, s, _ in FILL for g in range(G) if (f, g) not in filled and at[g] > after[f]
            ]
            if not spare:
                now = min(ready[g] for g in range(G) if at[g] < len(CHAIN))
                continue
            g, name = min(spare, key=lambda s: (s[1] != "early", s[0]))
        order.append((name, g))
        if name in after:
            filled.add((name, g))
            now += [c for f, _, c in FILL if f == name][0]
            continue
        _, cost, link, way = CHAIN[at[g]]
        now += cost
        at[g] += 1
        ready[g] = now
        if link:
            links[link] = max(now, links[link]) + BUSY[link]
            ready[g] = links[link] + way
    return order, now


def cols(head):
    return pl.ds(pl.multiple_of(head * D, D), D)


def mm(a, b, da, db):
    return lax.dot_general(a, b, (((da,), (db,)), ((), ())), preferred_element_type=F32)


def kernel(q, k, v, g_out, log_decay, gain, out, gq, gk, gv, gain_sum, *refs):
    nd, ns, ng = len(Decays.scratch), len(Scan.scratch), len(Gain.scratch)
    total, cum, cums, inside, wts, ga, gkp, gvp, part, local, prior, later_local, later = refs[:13]
    refs = refs[13:]
    me = here()
    decays = Decays(me, refs[:nd], total)
    refs = refs[nd:]
    fore = Scan(me, refs[:ns], decays, prior, False)
    back = Scan(me, refs[ns : 2 * ns], decays, later, True)
    sums = Gain(me, refs[2 * ns :], part, gain_sum)

    met = greet(me)
    upper = (
        lax.broadcasted_iota(jnp.int32, (T, T), 0) <= lax.broadcasted_iota(jnp.int32, (T, T), 1)
    ).astype(F32)
    running = lax.dot_general(
        log_decay[...], upper, (((1,), (0,)), ((), ())), precision=lax.Precision.HIGHEST, preferred_element_type=F32
    )
    cum[...] = running
    blocks = jnp.broadcast_to(running[:, T - 1 : T], (HEADS, D))
    for j in range(NY):
        total[j] = blocks[j * OWN : (j + 1) * OWN]

    def for_heads(g, work):
        def step(d, carry):
            j = lax.rem(me["y"] + 1 + d, NY)
            for i in range(HPG):
                work(j, i, j * OWN + g * HPG + i)
            return carry

        lax.fori_loop(0, NY, step, 0)

    def weight(head):
        by_row = cums[head]
        gap = jnp.concatenate([by_row, by_row[:, : T - D]], axis=1) - cum[pl.ds(head, 1), :]
        causal = lax.broadcasted_iota(jnp.int32, (T, T), 0) >= lax.broadcasted_iota(jnp.int32, (T, T), 1)
        return jnp.exp(jnp.where(causal, gap, -1e30))

    def end_scale(head):
        by_row = cums[head]
        return jnp.exp(by_row[T - 1 : T, :] - by_row)

    def local_of(g):
        def work(j, i, head):
            by_row = jnp.transpose(jnp.broadcast_to(cum[pl.ds(head, 1), :], (D, T)))
            cums[head] = by_row
            scale = jnp.exp(by_row[T - 1 : T, :] - by_row)
            decayed = (k[:, cols(head)].astype(F32) * scale).astype(BF)
            local[j, g, pl.ds(i * D, D), :] = mm(decayed, v[:, cols(head)], 0, 0).astype(BF)

        for_heads(g, work)
        fore.yin[NY - 1, g] = local[me["y"], g]

    def early(g):
        def work(j, i, head):
            scores = mm(q[:, cols(head)], k[:, cols(head)], 1, 1)
            weighted = (scores * weight(head)).astype(BF)
            wts[head] = weighted
            inside[head] = mm(weighted, v[:, cols(head)], 1, 0)

        for_heads(g, work)

    def middle(g):
        for step in fore.yback.steps:
            fore.arrive(g, step)

        def work(j, i, head):
            state = prior[j, g, pl.ds(i * D, D), :]
            start = jnp.exp(cums[head])
            qh = q[:, cols(head)]
            attended = inside[head] + mm(qh, state, 1, 0) * start
            inv = lax.rsqrt(jnp.mean(attended * attended, axis=1, keepdims=True) + epsilon)
            normed = attended * inv
            row = gain[pl.ds(head, 1), :]
            out[:, cols(head)] = (normed * row).astype(BF)
            grad = g_out[:, cols(head)].astype(F32)
            scaled = grad * row
            lean = jnp.mean(scaled * normed, axis=1, keepdims=True)
            attended_grad = (inv * (scaled - normed * lean)).astype(BF)
            ga[head] = attended_grad
            part[head] = jnp.sum((grad * normed).reshape(T // 8, 8, D), axis=0)
            decayed = (qh.astype(F32) * start).astype(BF)
            later_local[j, g, pl.ds(i * D, D), :] = mm(decayed, attended_grad, 0, 0).astype(BF)

        for_heads(g, work)
        back.start(g, lambda peer: later_local.at[peer, g])
        back.yin[NY - 1, g] = later_local[me["y"], g]

    def late(g):
        def work(j, i, head):
            grad = ga[head]
            grad_scores = mm(grad, v[:, cols(head)], 1, 1)
            gw = (grad_scores * weight(head)).astype(BF)
            state = prior[j, g, pl.ds(i * D, D), :]
            gq[:, cols(head)] = (mm(gw, k[:, cols(head)], 1, 0) + jnp.exp(cums[head]) * mm(grad, state, 1, 1)).astype(BF)
            gkp[head] = mm(gw, q[:, cols(head)], 0, 0)
            gvp[head] = mm(wts[head], grad, 0, 0)

        for_heads(g, work)

    def last(g):
        for step in back.yback.steps:
            back.arrive(g, step)

        def work(j, i, head):
            state = later[j, g, pl.ds(i * D, D), :]
            scale = end_scale(head)
            gk[:, cols(head)] = (gkp[head] + scale * mm(v[:, cols(head)], state, 1, 1)).astype(BF)
            gv[:, cols(head)] = (gvp[head] + scale * mm(k[:, cols(head)], state, 1, 0)).astype(BF)

        for_heads(g, work)

    stages = {
        "early": early,
        "lines": fore.over_lines,
        "planes": fore.over_planes,
        "before_lines": fore.before_lines,
        "before_blocks": fore.before_blocks,
        "middle": middle,
        "late": late,
        "back_lines": back.over_lines,
        "back_planes": back.over_planes,
        "back_before_lines": back.before_lines,
        "back_before_blocks": back.before_blocks,
        "last": last,
    }
    order, _ = plan()
    levels = [lambda: decays.lift("y", "x"), lambda: decays.lift("x", "z"), lambda: decays.settle("z")]
    needs = {"lines": 1, "planes": 2, "before_lines": 3}
    folds = [sums.over_z, sums.over_x, sums.over_y, sums.over_dp]
    to_open = True
    middles = 0
    for name, g in order:
        if name == "local":
            local_of(g)
            if to_open:
                met()
                decays.start()
                to_open = False
            fore.start(g, lambda peer: local.at[peer, g])
            continue
        while levels and needs.get(name, 0) > 3 - len(levels):
            levels.pop(0)()
        stages[name](g)
        if name == "middle":
            middles += 1
            if middles == G:
                sums.start()
        elif middles == G and folds and name == "back_before_lines":
            folds.pop(0)()
        elif middles == G and folds and name == "last":
            folds.pop(0)()
    for fold in folds:
        fold()
    decays.drain()
    fore.drain()
    back.drain()
    sums.drain()


def body(queries, key_vectors, value_vectors, out_grad, log_decay, norm_gain):
    shape = queries.shape
    wide = shape[-1]
    vmem = pl.BlockSpec(memory_space=pltpu.VMEM)
    scratch = [
        pltpu.VMEM((NY, OWN, D), F32),
        pltpu.VMEM((HEADS, T), F32),
        pltpu.VMEM((HEADS, T, D), F32),
        pltpu.VMEM((HEADS, T, D), F32),
        pltpu.VMEM((HEADS, T, T), BF),
        pltpu.VMEM((HEADS, T, D), BF),
        pltpu.VMEM((HEADS, T, D), F32),
        pltpu.VMEM((HEADS, T, D), F32),
        pltpu.VMEM((HEADS, 8, D), F32),
        pltpu.VMEM((NY, G, R, D), BF),
        pltpu.VMEM((NY, G, R, D), BF),
        pltpu.VMEM((NY, G, R, D), BF),
        pltpu.VMEM((NY, G, R, D), BF),
    ]
    rows = jax.ShapeDtypeStruct((T, wide), BF)
    results = pl.pallas_call(
        kernel,
        out_shape=[rows] * 4 + [jax.ShapeDtypeStruct((1, D // NY), F32)],
        in_specs=[vmem] * 6,
        out_specs=[vmem] * 5,
        scratch_shapes=scratch + Decays.scratch + Scan.scratch * 2 + Gain.scratch,
        compiler_params=pltpu.CompilerParams(
            collective_id=0, has_side_effects=True, vmem_limit_bytes=60 * 1024 * 1024
        ),
        name="attention",
    )(
        *[a.reshape(T, wide) for a in (queries, key_vectors, value_vectors, out_grad)],
        log_decay.reshape(HEADS, T),
        norm_gain.reshape(HEADS, D),
    )
    return (*[r.reshape(shape) for r in results[:4]], results[4].reshape(D // NY))


def solution(mesh):
    split = Mesh(mesh.devices.reshape(NZ, NX, NY, mesh.shape["dp"]), AXES)
    rows = P("dp", SEQ, None)
    return jax.shard_map(
        body,
        mesh=split,
        in_specs=(rows, rows, rows, rows, P("dp", None, SEQ), P()),
        out_specs=(rows, rows, rows, rows, P(SEQ)),
        check_vma=False,
    )
```

```python
import functools

import jax
import jax.numpy as jnp
from jax import lax
from jax.experimental import pallas as pl
from jax.experimental.pallas import tpu as pltpu
from jax.sharding import Mesh
from jax.sharding import PartitionSpec as P

AXES = ("z", "x", "y", "dp")
SEQ = ("z", "x", "y")
SIZES = {"z": 8, "x": 4, "y": 4, "dp": 2}
NZ, NX, NY = 8, 4, 4
D = 128
OWN = 8
G = 8
HPG = OWN // G
AT_ONCE = min(NY, 4 // HPG)
R = HPG * D
RX = R // NX
BF = jnp.bfloat16
F32 = jnp.float32
epsilon = 1e-06


def here():
    return {name: lax.axis_index(name) for name in AXES}


def shifted(me, axis, step):
    there = dict(me)
    there[axis] = lax.rem(me[axis] + step, SIZES[axis])
    return tuple(there[name] for name in AXES)


def push(src, dst, send, recv, target):
    return pltpu.make_async_remote_copy(
        src_ref=src,
        dst_ref=dst,
        send_sem=send,
        recv_sem=recv,
        device_id=target,
        device_id_type=pl.DeviceIdType.MESH,
    )


class Wire:
    def __init__(self, me, axis, sems):
        self.me, self.axis, self.sems = me, axis, sems
        self.peers = SIZES[axis] - 1
        self.sent = []

    def peer(self, step):
        return lax.rem(self.me[self.axis] + step, SIZES[self.axis])

    def send(self, key, source, slots):
        for step in range(1, self.peers + 1):
            push(
                source(self.peer(step)),
                slots.at[step - 1],
                self.sems[0].at[key],
                self.sems[1].at[key],
                shifted(self.me, self.axis, step),
            ).start()
        self.sent.append((key, slots))

    def _all(self, key, slots):
        taken = slots.at[pl.ds(0, self.peers)]
        return push(taken, taken, self.sems[0].at[key], self.sems[1].at[key], shifted(self.me, self.axis, 1))

    def arrived(self, key, slots):
        self._all(key, slots).wait_recv()

    def drain(self):
        for key, slots in self.sent:
            self._all(key, slots).wait_send()
        self.sent = []


def sem_pair(keys):
    return [pltpu.SemaphoreType.DMA((keys,))] * 2


def slot_of(me, axis, index):
    n = SIZES[axis]
    return lax.rem(me[axis] + (n - 1) + (n - index), n)


def greet(me):
    barrier = pltpu.get_barrier_semaphore()
    count = 0
    for axis in AXES:
        for step in range(1, SIZES[axis]):
            pl.semaphore_signal(
                barrier, inc=1, device_id=shifted(me, axis, step), device_id_type=pl.DeviceIdType.MESH
            )
            count += 1
    return lambda: pl.semaphore_wait(barrier, count)


class Decays:
    scratch = [
        pltpu.VMEM((NY, OWN, D), F32),
        pltpu.VMEM((NX, OWN, D), F32),
        pltpu.VMEM((NZ, OWN, D), F32),
        *sem_pair(1) * 3,
    ]

    def __init__(self, me, refs, total):
        self.me, self.total = me, total
        self.levels = dict(zip("yxz", refs[:3]))
        self.wires = {a: Wire(me, a, refs[3 + 2 * i : 5 + 2 * i]) for i, a in enumerate("yxz")}

    def start(self):
        level = self.levels["y"]
        self.wires["y"].send(0, lambda peer: self.total.at[peer], level)
        level[NY - 1] = self.total[self.me["y"]]

    def settle(self, axis):
        self.wires[axis].arrived(0, self.levels[axis])

    def lift(self, low, high):
        self.settle(low)
        n, m = SIZES[low], SIZES[high]
        level, above = self.levels[low], self.levels[high]
        above[m - 1] = functools.reduce(jnp.add, [level[slot_of(self.me, low, k)] for k in range(n)])
        self.wires[high].send(0, lambda peer: above.at[m - 1], above)

    def row(self, axis, slot, head):
        return jnp.exp(self.levels[axis][slot, pl.ds(head, 1), :])

    def drain(self):
        for wire in self.wires.values():
            wire.drain()


class Scan:
    scratch = [
        pltpu.VMEM((G, NY, R, D), BF),
        pltpu.VMEM((G, NX, RX, D), BF),
        pltpu.VMEM((G, NX, RX, D), BF),
        pltpu.VMEM((G, NZ, RX, D), BF),
        pltpu.VMEM((G, NX, RX, D), BF),
        pltpu.VMEM((G, NX, RX, D), BF),
        pltpu.VMEM((G, NY, R, D), BF),
        *sem_pair(G) * 5,
    ]

    def __init__(self, me, refs, decays, prior, backward):
        self.me, self.decays, self.prior, self.backward = me, decays, prior, backward
        self.yin, self.xin, self.xout, self.zin, self.lines, self.line, self.yout = refs[:7]
        sems = refs[7:]
        names = ("y", "x", "z", "x", "y")
        self.y, self.x, self.z, self.xback, self.yback = [
            Wire(me, a, sems[2 * i : 2 * i + 2]) for i, a in enumerate(names)
        ]

    def order(self, n):
        return list(range(n))[:: -1 if self.backward else 1]

    def start(self, g, states):
        self.y.send(g, lambda peer: states.at[peer, g], self.yin.at[g])
        self.yin[g, NY - 1] = states[self.me["y"], g]

    def over_lines(self, g):
        me = self.me
        self.y.arrived(g, self.yin.at[g])
        for i in range(HPG):
            rows = pl.ds(i * D, D)
            total = None
            for k in self.order(NY):
                slot = slot_of(me, "y", k)
                term = self.yin[g, slot, rows, :].astype(F32)
                total = term if total is None else total * self.decays.row("y", slot, g * HPG + i) + term
            total = total.astype(BF)
            if RX >= D:
                per = RX // D
                self.xout[g, i // per, pl.ds((i % per) * D, D), :] = total
            else:
                per = D // RX
                for j in range(per):
                    self.xout[g, i * per + j] = total[j * RX : (j + 1) * RX]
        self.x.send(g, lambda peer: self.xout.at[g, peer], self.xin.at[g])
        self.xin[g, NX - 1] = self.xout[g, me["x"]]

    def pieces(self, g):
        first = g * HPG + (self.me["x"] * RX) // D
        return [(first + i, pl.ds(i * D, min(D, RX))) for i in range(max(1, RX // D))]

    def over_planes(self, g):
        me = self.me
        self.x.arrived(g, self.xin.at[g])
        for head, rows in self.pieces(g):
            total = None
            for k in self.order(NX):
                slot = slot_of(me, "x", k)
                term = self.xin[g, slot, rows, :].astype(F32)
                total = term if total is None else total * self.decays.row("x", slot, head) + term
            self.zin[g, NZ - 1, rows, :] = total.astype(BF)
        self.z.send(g, lambda peer: self.zin.at[g, NZ - 1], self.zin.at[g])

    def before_lines(self, g):
        me = self.me
        self.z.arrived(g, self.zin.at[g])
        for head, rows in self.pieces(g):
            state = jnp.zeros((min(D, RX), D), F32)
            for k in self.order(NZ):
                slot = slot_of(me, "z", k)
                passed = (k > me["z"]) if self.backward else (k < me["z"])
                ahead = state * self.decays.row("z", slot, head) + self.zin[g, slot, rows, :].astype(F32)
                state = jnp.where(passed, ahead, state)
            for n, k in enumerate(self.order(NX)):
                self.lines[g, k, rows, :] = state.astype(BF)
                if n < NX - 1:
                    slot = slot_of(me, "x", k)
                    state = state * self.decays.row("x", slot, head) + self.xin[g, slot, rows, :].astype(F32)
        self.xback.send(g, lambda peer: self.lines.at[g, peer], self.line.at[g])
        self.line[g, NX - 1] = self.lines[g, me["x"]]

    def before_blocks(self, g):
        me = self.me
        self.xback.arrived(g, self.line.at[g])
        for i in range(HPG):
            rows = pl.ds(i * D, D)
            if RX >= D:
                per = RX // D
                slot = slot_of(me, "x", i // per)
                state = self.line[g, slot, pl.ds((i % per) * D, D), :].astype(F32)
            else:
                per = D // RX
                state = jnp.concatenate(
                    [self.line[g, slot_of(me, "x", i * per + j)].astype(F32) for j in range(per)], axis=0
                )
            for n, k in enumerate(self.order(NY)):
                self.yout[g, k, rows, :] = state.astype(BF)
                if n < NY - 1:
                    slot = slot_of(me, "y", k)
                    row = self.decays.row("y", slot, g * HPG + i)
                    state = state * row + self.yin[g, slot, rows, :].astype(F32)
        self.yback.send(g, lambda peer: self.yout.at[g, peer], self.prior.at[g])
        self.prior[g, NY - 1] = self.yout[g, me["y"]]

    def arrive(self, g):
        self.yback.arrived(g, self.prior.at[g])

    def drain(self):
        for wire in (self.y, self.x, self.z, self.xback, self.yback):
            wire.drain()


class Gain:
    AXES = ("z", "x", "y", "dp")
    scratch = [*[pltpu.VMEM((SIZES[a], 8, D), F32) for a in AXES], *sem_pair(1) * 4]

    def __init__(self, me, refs, part, out):
        self.me, self.part, self.out = me, part, out
        self.levels = dict(zip(self.AXES, refs[:4]))
        self.wires = {a: Wire(me, a, refs[4 + 2 * i : 6 + 2 * i]) for i, a in enumerate(self.AXES)}

    def start(self):
        self.wires["z"].send(0, lambda peer: self.part.at[peer], self.levels["z"])
        self.levels["z"][NZ - 1] = self.part[self.me["z"]]

    def fold(self, axis):
        n, level = SIZES[axis], self.levels[axis]
        self.wires[axis].arrived(0, level)
        total = functools.reduce(jnp.add, [level[slot_of(self.me, axis, k)] for k in range(n)])
        if axis != "dp":
            above = self.AXES[self.AXES.index(axis) + 1]
            held, m = self.levels[above], SIZES[above]
            held[m - 1] = total
            self.wires[above].send(0, lambda peer: held.at[m - 1], held)
            return
        width = D // NY
        mine = lax.broadcasted_iota(jnp.int32, (8, D), 0) == self.me["x"]
        row = jnp.sum(jnp.where(mine, total, 0.0), axis=0, keepdims=True)
        self.out[...] = functools.reduce(
            jnp.add,
            [jnp.where(self.me["y"] == k, row[:, k * width : (k + 1) * width], 0.0) for k in range(NY)],
        )

    def drain(self):
        for wire in self.wires.values():
            wire.drain()


T = 192
HEADS = NY * OWN

PER = 4 / G
CHAIN = (
    ("local", 0.87 * PER, "y", 4.9),
    ("lines", 0.06, "x", 4.5),
    ("planes", 0.06, "z", 4.3),
    ("before_lines", 0.07, "x", 3.3),
    ("before_blocks", 0.07, "y", 2.4),
    ("middle", 2.1 * PER, "y", 4.2),
    ("back_lines", 0.06, "x", 4.5),
    ("back_planes", 0.06, "z", 4.3),
    ("back_before_lines", 0.07, "x", 3.5),
    ("back_before_blocks", 0.07, "y", 2.8),
    ("last", 0.6 * PER, None, 0.0),
)
BUSY = {"y": 11.3 / G, "x": 2.9 / G, "z": 11.3 / G}
EARLY, LATE = (1, 2) if G > 4 else (2, 2)
FILL = {f"early{n}": ("middle", 1.1 * PER / EARLY) for n in range(EARLY)} | {
    f"late{n}": ("last", 2.7 * PER / LATE) for n in range(LATE)
}
GAIN = (("gain", 4.8), ("gain_z", 4.0), ("gain_x", 4.0), ("gain_y", 2.0), ("gain_dp", 0.0))
MARGIN = 2.0


def plan():
    rest = [sum(c[1] + c[3] for c in CHAIN[i:]) for i in range(len(CHAIN))]
    step_of = {c[0]: i for i, c in enumerate(CHAIN)}
    now, at, ready = 0.0, [0] * G, [0.0] * G
    links = {"y": 0.0, "x": 0.0, "z": 0.0}
    filled, order = set(), []
    summed, sums_ready = 0, None
    while any(a < len(CHAIN) for a in at):
        fits = []
        for g in range(G):
            if at[g] < len(CHAIN) and ready[g] <= now:
                name = CHAIN[at[g]][0]
                lacking = [f for f in FILL if FILL[f][0] == name and (f, g) not in filled]
                fits.append((-rest[at[g]], g, lacking[0] if lacking else name))
        if fits:
            _, g, name = min(fits)
        elif sums_ready is not None and summed < len(GAIN) and sums_ready <= now:
            order.append((GAIN[summed][0], 0))
            sums_ready = now + GAIN[summed][1] + MARGIN
            summed += 1
            now += 0.1
            continue
        else:
            soon = min(ready[g] for g in range(G) if at[g] < len(CHAIN))
            spare = [
                (not f.startswith("early"), g, f)
                for f in FILL
                for g in range(G)
                if (f, g) not in filled and at[g] > (0 if f.startswith("early") else step_of["middle"])
                if now + FILL[f][1] <= soon + 0.15
            ]
            if not spare:
                now = soon
                continue
            _, g, name = min(spare)
        order.append((name, g))
        if name in FILL:
            filled.add((name, g))
            now += FILL[name][1]
            continue
        _, cost, link, way = CHAIN[at[g]]
        now += cost
        at[g] += 1
        ready[g] = now
        if link:
            links[link] = max(now, links[link]) + BUSY[link]
            ready[g] = links[link] + way
        if all(a > step_of["middle"] for a in at) and sums_ready is None:
            sums_ready = now
    order += [(name, 0) for name, _ in GAIN[summed:]]
    return order, now


def cols(head):
    return pl.ds(pl.multiple_of(head * D, D), D)


def mm(a, b, da, db):
    return lax.dot_general(a, b, (((da,), (db,)), ((), ())), preferred_element_type=F32)


def kernel(*refs):
    sources, (out, gq, gk, gv, gain_sum), refs = refs[:6], refs[6:11], refs[11:]
    (q, k, v, g_out, log_decay, gain, in_sems), refs = refs[:7], refs[7:]
    nd, ns, ng = len(Decays.scratch), len(Scan.scratch), len(Gain.scratch)
    total, cum, cums, inside, wts, weights, ga, gkp, gvp, gain_part, local, prior, later_local, later = refs[:14]
    refs = refs[14:]
    me = here()
    decays = Decays(me, refs[:nd], total)
    refs = refs[nd:]
    fore = Scan(me, refs[:ns], decays, prior, False)
    back = Scan(me, refs[ns : 2 * ns], decays, later, True)
    sums = Gain(me, refs[2 * ns :], gain_part, gain_sum)

    met = greet(me)
    held = (q, k, v, g_out, log_decay, gain)
    loads = [pltpu.make_async_copy(a, b, in_sems.at[n]) for n, (a, b) in enumerate(zip(sources, held))]
    for n in (4, 1, 2, 0, 3, 5):
        loads[n].start()
    loads[4].wait()
    upper = (
        lax.broadcasted_iota(jnp.int32, (T, T), 0) <= lax.broadcasted_iota(jnp.int32, (T, T), 1)
    ).astype(F32)
    running = lax.dot_general(
        log_decay[...], upper, (((1,), (0,)), ((), ())), precision=lax.Precision.HIGHEST, preferred_element_type=F32
    )
    cum[...] = running
    gain_part[...] = jnp.zeros_like(gain_part)
    blocks = jnp.broadcast_to(running[:, T - 1 : T], (HEADS, D))
    for j in range(NY):
        total[j] = blocks[j * OWN : (j + 1) * OWN]

    def for_heads(g, work, begin=0, end=NY, at_once=AT_ONCE):
        at_once = min(at_once, end - begin)

        def step(n, carry):
            for u in range(at_once):
                j = lax.rem(me["y"] + 1 + begin + n * at_once + u, NY)
                for i in range(HPG):
                    work(j, i, j * OWN + g * HPG + i)
            return carry

        if end - begin == at_once:
            step(0, 0)
        else:
            lax.fori_loop(0, (end - begin) // at_once, step, 0)

    def weight(head):
        by_row = cums[head]
        gap = jnp.concatenate([by_row, by_row[:, : T - D]], axis=1) - cum[pl.ds(head, 1), :]
        causal = lax.broadcasted_iota(jnp.int32, (T, T), 0) >= lax.broadcasted_iota(jnp.int32, (T, T), 1)
        return jnp.exp(jnp.where(causal, gap, -1e30))

    def end_scale(head):
        by_row = cums[head]
        return jnp.exp(by_row[T - 1 : T, :] - by_row)

    def local_of(g):
        def work(j, i, head):
            by_row = jnp.transpose(jnp.broadcast_to(cum[pl.ds(head, 1), :], (D, T)))
            cums[head] = by_row
            scale = jnp.exp(by_row[T - 1 : T, :] - by_row)
            decayed = (k[:, cols(head)].astype(F32) * scale).astype(BF)
            local[j, g, pl.ds(i * D, D), :] = mm(decayed, v[:, cols(head)], 0, 0).astype(BF)

        for_heads(g, work)

    def early(part, g):
        def work(j, i, head):
            scores = mm(q[:, cols(head)], k[:, cols(head)], 1, 1)
            factor = weight(head)
            weights[head] = factor
            weighted = (scores * factor).astype(BF)
            wts[head] = weighted
            inside[head] = mm(weighted, v[:, cols(head)], 1, 0)

        for_heads(g, work, NY // EARLY * part, NY // EARLY * (part + 1))

    def middle(g):
        fore.arrive(g)

        def work(j, i, head):
            state = prior[g, slot_of(me, "y", j), pl.ds(i * D, D), :]
            start = jnp.exp(cums[head])
            qh = q[:, cols(head)]
            attended = inside[head] + mm(qh, state, 1, 0) * start
            inv = lax.rsqrt(jnp.mean(attended * attended, axis=1, keepdims=True) + epsilon)
            normed = attended * inv
            row = gain[pl.ds(head, 1), :]
            out[:, cols(head)] = (normed * row).astype(BF)
            grad = g_out[:, cols(head)].astype(F32)
            scaled = grad * row
            lean = jnp.mean(scaled * normed, axis=1, keepdims=True)
            attended_grad = (inv * (scaled - normed * lean)).astype(BF)
            ga[head] = attended_grad
            gain_part[head // 4, pl.ds(lax.rem(head, 4), 1), :] = jnp.sum(grad * normed, axis=0, keepdims=True)
            decayed = (qh.astype(F32) * start).astype(BF)
            later_local[j, g, pl.ds(i * D, D), :] = mm(decayed, attended_grad, 0, 0).astype(BF)

        for_heads(g, work)
        back.start(g, later_local)

    def late(part, g):
        def work(j, i, head):
            grad = ga[head]
            grad_scores = mm(grad, v[:, cols(head)], 1, 1)
            gw = (grad_scores * weights[head]).astype(BF)
            state = prior[g, slot_of(me, "y", j), pl.ds(i * D, D), :]
            gq[:, cols(head)] = (mm(gw, k[:, cols(head)], 1, 0) + jnp.exp(cums[head]) * mm(grad, state, 1, 1)).astype(BF)
            gkp[head] = mm(gw, q[:, cols(head)], 0, 0)
            gvp[head] = mm(wts[head], grad, 0, 0)

        for_heads(g, work, NY // LATE * part, NY // LATE * (part + 1))

    def last(g):
        back.arrive(g)

        def work(j, i, head):
            state = later[g, slot_of(me, "y", j), pl.ds(i * D, D), :]
            scale = end_scale(head)
            gk[:, cols(head)] = (gkp[head] + scale * mm(v[:, cols(head)], state, 1, 1)).astype(BF)
            gv[:, cols(head)] = (gvp[head] + scale * mm(k[:, cols(head)], state, 1, 0)).astype(BF)

        for_heads(g, work)

    stages = {
        "lines": fore.over_lines,
        "planes": fore.over_planes,
        "before_lines": fore.before_lines,
        "before_blocks": fore.before_blocks,
        "middle": middle,
        "back_lines": back.over_lines,
        "back_planes": back.over_planes,
        "back_before_lines": back.before_lines,
        "back_before_blocks": back.before_blocks,
        "last": last,
    }
    for n in range(EARLY):
        stages[f"early{n}"] = functools.partial(early, n)
    for n in range(LATE):
        stages[f"late{n}"] = functools.partial(late, n)
    stages["gain"] = lambda g: sums.start()
    for axis in sums.AXES:
        stages[f"gain_{axis}"] = lambda g, axis=axis: sums.fold(axis)
    order, _ = plan()
    levels = [lambda: decays.lift("y", "x"), lambda: decays.lift("x", "z"), lambda: decays.settle("z")]
    needs = {"lines": 1, "planes": 2, "before_lines": 3}
    to_open = True
    loads[1].wait()
    loads[2].wait()
    for name, g in order:
        if name == "local":
            local_of(g)
            if to_open:
                met()
                decays.start()
                to_open = False
            fore.start(g, local)
            continue
        if name.startswith("early") and loads[0]:
            loads[0].wait()
            loads[0] = None
        if name == "middle" and loads[3]:
            loads[3].wait()
            loads[5].wait()
            loads[3] = None
        while levels and needs.get(name, 0) > 3 - len(levels):
            levels.pop(0)()
        stages[name](g)
        if name == "gain":
            fore.drain()
            decays.drain()
    back.drain()
    sums.drain()


PARTS = 4


def store_kernel(*refs):
    given, kept, sems = refs[:5], refs[5:10], refs[10]
    copies = [pltpu.make_async_copy(given[4], kept[4], sems.at[4 * PARTS])]
    for n in range(4):
        for p in range(PARTS):
            rows = pl.ds(p * (T // PARTS), T // PARTS)
            copies.append(pltpu.make_async_copy(given[n].at[rows], kept[n].at[rows], sems.at[n * PARTS + p]))
    for copy in copies:
        copy.start()
    for copy in copies:
        copy.wait()


def body(queries, key_vectors, value_vectors, out_grad, log_decay, norm_gain):
    shape = queries.shape
    wide = shape[-1]
    vmem = pl.BlockSpec(memory_space=pltpu.VMEM)
    scratch = [
        pltpu.VMEM((NY, OWN, D), F32),
        pltpu.VMEM((HEADS, T), F32),
        pltpu.VMEM((HEADS, T, D), F32),
        pltpu.VMEM((HEADS, T, D), F32),
        pltpu.VMEM((HEADS, T, T), BF),
        pltpu.VMEM((HEADS, T, T), F32),
        pltpu.VMEM((HEADS, T, D), BF),
        pltpu.VMEM((HEADS, T, D), F32),
        pltpu.VMEM((HEADS, T, D), F32),
        pltpu.VMEM((NZ, 8, D), F32),
        pltpu.VMEM((NY, G, R, D), BF),
        pltpu.VMEM((G, NY, R, D), BF),
        pltpu.VMEM((NY, G, R, D), BF),
        pltpu.VMEM((G, NY, R, D), BF),
    ]
    rows = (T, wide)
    last_row = (1, D // NY)
    hbm = pl.BlockSpec(memory_space=pltpu.HBM)
    results = pl.pallas_call(
        kernel,
        out_shape=[pltpu.VMEM(rows, BF)] * 4 + [pltpu.VMEM(last_row, F32)],
        in_specs=[hbm] * 6,
        out_specs=[vmem] * 5,
        scratch_shapes=[
            *[pltpu.VMEM(rows, BF)] * 4,
            pltpu.VMEM((HEADS, T), F32),
            pltpu.VMEM((HEADS, D), F32),
            pltpu.SemaphoreType.DMA((6,)),
            *scratch,
            *Decays.scratch,
            *Scan.scratch,
            *Scan.scratch,
            *Gain.scratch,
        ],
        compiler_params=pltpu.CompilerParams(
            collective_id=0, has_side_effects=True, vmem_limit_bytes=48 * 1024 * 1024
        ),
        name="attention",
    )(
        *[a.reshape(rows) for a in (queries, key_vectors, value_vectors, out_grad)],
        log_decay.reshape(HEADS, T),
        norm_gain.reshape(HEADS, D),
    )
    results = pl.pallas_call(
        store_kernel,
        out_shape=[jax.ShapeDtypeStruct(rows, BF)] * 4 + [jax.ShapeDtypeStruct(last_row, F32)],
        in_specs=[vmem] * 5,
        out_specs=[hbm] * 5,
        scratch_shapes=[pltpu.SemaphoreType.DMA((4 * PARTS + 1,))],
        compiler_params=pltpu.CompilerParams(vmem_limit_bytes=1024 * 1024),
        name="store",
    )(*results)
    return (*[r.reshape(shape) for r in results[:4]], results[4].reshape(D // NY))


def solution(mesh):
    split = Mesh(mesh.devices.reshape(NZ, NX, NY, mesh.shape["dp"]), AXES)
    rows = P("dp", SEQ, None)
    return jax.shard_map(
        body,
        mesh=split,
        in_specs=(rows, rows, rows, rows, P("dp", None, SEQ), P()),
        out_specs=(rows, rows, rows, rows, P(SEQ)),
        check_vma=False,
    )
```

```python
import functools

import jax
import jax.numpy as jnp
from jax import lax
from jax.experimental import pallas as pl
from jax.experimental.pallas import tpu as pltpu
from jax.sharding import Mesh
from jax.sharding import PartitionSpec as P

AXES = ("z", "x", "y", "dp")
SEQ = ("z", "x", "y")
SIZES = {"z": 8, "x": 4, "y": 4, "dp": 2}
NZ, NX, NY = 8, 4, 4
NP = NX * NY
D = 128
T = 192
HEADS = 2 * NP
NR = 2
RR = D // NR
UNITS = 2 * NR
BATCHES = 4
PER = NP // BATCHES
BF = jnp.bfloat16
F32 = jnp.float32
epsilon = 1e-06


def here():
    return {name: lax.axis_index(name) for name in AXES}


def plane_index(me):
    return me["x"] * NY + me["y"]


def shifted(me, **steps):
    return tuple(lax.rem(me[a] + steps[a], SIZES[a]) if a in steps else me[a] for a in AXES)


def push(src, dst, send, recv, target):
    return pltpu.make_async_remote_copy(
        src_ref=src,
        dst_ref=dst,
        send_sem=send,
        recv_sem=recv,
        device_id=target,
        device_id_type=pl.DeviceIdType.MESH,
    )


class Wire:
    def __init__(self, me, axis, sems):
        self.me, self.axis, self.sems = me, axis, sems
        self.peers = (NP if axis == "plane" else SIZES[axis]) - 1
        self.sent = {}

    def target(self, step):
        if self.axis == "plane":
            return shifted(self.me, x=step // NY, y=step % NY)
        return shifted(self.me, **{self.axis: step})

    def peer(self, step):
        to = self.target(step)
        if self.axis == "plane":
            return to[1] * NY + to[2]
        return to[AXES.index(self.axis)]

    def send(self, key, source, slots, steps=None):
        for step in steps or range(1, self.peers + 1):
            push(
                source(self.peer(step)),
                slots.at[step - 1],
                self.sems[0].at[key],
                self.sems[1].at[key],
                self.target(step),
            ).start()
        self.sent[key] = slots

    def _all(self, key, slots):
        taken = slots.at[pl.ds(0, self.peers)]
        return push(taken, taken, self.sems[0].at[key], self.sems[1].at[key], self.target(1))

    def arrived(self, key, slots):
        self._all(key, slots).wait_recv()

    def drain(self):
        for key, slots in self.sent.items():
            self._all(key, slots).wait_send()
        self.sent = {}


def sem_pair(keys):
    return [pltpu.SemaphoreType.DMA((keys,))] * 2


def slot_of(me, axis, index):
    if axis == "plane":
        dx = lax.rem(me["x"] + (NX - index // NY), NX)
        dy = lax.rem(me["y"] + (NY - index % NY), NY)
        return lax.rem(dx * NY + dy + (NP - 1), NP)
    n = SIZES[axis]
    return lax.rem(me[axis] + (n - 1) + (n - index), n)


def greet(me):
    barrier = pltpu.get_barrier_semaphore()
    targets = [shifted(me, z=step) for step in range(1, NZ)]
    targets += [shifted(me, x=step // NY, y=step % NY) for step in range(1, NP)]
    targets.append(shifted(me, dp=1))
    for target in targets:
        pl.semaphore_signal(barrier, inc=1, device_id=target, device_id_type=pl.DeviceIdType.MESH)
    return lambda: pl.semaphore_wait(barrier, len(targets))


class Decays:
    scratch = [*[pltpu.VMEM((n, 8, D), F32) for n in (NP, NZ, NP, NZ)], *sem_pair(1) * 2]

    def __init__(self, me, refs, total):
        self.me, self.total = me, total
        self.logs = {"plane": refs[0], "z": refs[1]}
        self.factors = {"plane": refs[2], "z": refs[3]}
        self.wires = {a: Wire(me, a, refs[4 + 2 * i : 6 + 2 * i]) for i, a in enumerate(("plane", "z"))}

    def start(self):
        logs = self.logs["plane"]
        self.wires["plane"].send(0, lambda peer: self.total.at[peer], logs)
        logs[NP - 1] = self.total[plane_index(self.me)]

    def lift(self):
        logs, above = self.logs["plane"], self.logs["z"]
        self.wires["plane"].arrived(0, logs)
        above[NZ - 1] = functools.reduce(jnp.add, [logs[k] for k in range(NP)])
        self.wires["z"].send(0, lambda peer: above.at[NZ - 1], above)
        self.factors["plane"][...] = jnp.exp(logs[...])

    def settle(self):
        self.wires["z"].arrived(0, self.logs["z"])
        self.factors["z"][...] = jnp.exp(self.logs["z"][...])

    def row(self, axis, slot, turn):
        return self.factors[axis][slot, turn : turn + 1, :]

    def drain(self):
        for wire in self.wires.values():
            wire.drain()


class Scan:
    scratch = [
        pltpu.VMEM((UNITS, NP, RR, D), BF),
        pltpu.VMEM((UNITS, NZ, RR, D), BF),
        pltpu.VMEM((UNITS, NP, RR, D), BF),
        *sem_pair(UNITS) * 3,
    ]

    def __init__(self, me, refs, decays, states, prior, backward):
        self.me, self.decays, self.states, self.prior, self.backward = me, decays, states, prior, backward
        self.given, self.planes, self.before = refs[:3]
        self.plane, self.z, self.back = [
            Wire(me, a, refs[3 + 2 * i : 5 + 2 * i]) for i, a in enumerate(("plane", "z", "plane"))
        ]

    def order(self, n):
        return list(range(n))[:: -1 if self.backward else 1]

    def mine(self, u, owner):
        return self.states.at[owner, u // NR, pl.ds(u % NR * RR, RR)]

    def start(self, u, steps):
        sent = [step for step in steps if step < NP]
        self.plane.send(u, lambda owner: self.mine(u, owner), self.given.at[u], sent)
        if len(sent) < len(steps):
            self.given[u, NP - 1] = self.states[plane_index(self.me), u // NR, pl.ds(u % NR * RR, RR), :]

    def over_plane(self, u):
        self.plane.arrived(u, self.given.at[u])
        total = None
        for k in self.order(NP):
            slot = slot_of(self.me, "plane", k)
            term = self.given[u, slot].astype(F32)
            total = term if total is None else total * self.decays.row("plane", slot, u // NR) + term
        self.planes[u, NZ - 1] = total.astype(BF)
        self.z.send(u, lambda peer: self.planes.at[u, NZ - 1], self.planes.at[u])

    def before_blocks(self, u):
        me = self.me
        self.z.arrived(u, self.planes.at[u])
        state = jnp.zeros((RR, D), F32)
        for k in self.order(NZ):
            slot = slot_of(me, "z", k)
            passed = (k > me["z"]) if self.backward else (k < me["z"])
            ahead = state * self.decays.row("z", slot, u // NR) + self.planes[u, slot].astype(F32)
            state = jnp.where(passed, ahead, state)
        for n, k in enumerate(self.order(NP)):
            self.before[u, k] = state.astype(BF)
            if n < NP - 1:
                slot = slot_of(me, "plane", k)
                state = state * self.decays.row("plane", slot, u // NR) + self.given[u, slot].astype(F32)
        self.back.send(u, lambda peer: self.before.at[u, peer], self.prior.at[u])
        self.prior[u, NP - 1] = self.before[u, plane_index(me)]

    def arrive(self, turn):
        for u in range(turn * NR, (turn + 1) * NR):
            self.back.arrived(u, self.prior.at[u])

    def state(self, turn, owner):
        slot = slot_of(self.me, "plane", owner)
        parts = [self.prior[turn * NR + r, slot] for r in range(NR)]
        return jnp.concatenate(parts, axis=0)

    def drain(self):
        for wire in (self.plane, self.z, self.back):
            wire.drain()


class Gain:
    AXES = ("z", "x", "y", "dp")
    scratch = [*[pltpu.VMEM((SIZES[a], 8, D), F32) for a in AXES], *sem_pair(1) * 4]

    def __init__(self, me, refs, part, out):
        self.me, self.part, self.out = me, part, out
        self.levels = dict(zip(self.AXES, refs[:4]))
        self.wires = {a: Wire(me, a, refs[4 + 2 * i : 6 + 2 * i]) for i, a in enumerate(self.AXES)}

    def start(self):
        self.wires["z"].send(0, lambda peer: self.part.at[peer], self.levels["z"])
        self.levels["z"][NZ - 1] = self.part[self.me["z"]]

    def fold(self, axis):
        n, level = SIZES[axis], self.levels[axis]
        self.wires[axis].arrived(0, level)
        total = functools.reduce(jnp.add, [level[slot_of(self.me, axis, k)] for k in range(n)])
        if axis != "dp":
            above = self.AXES[self.AXES.index(axis) + 1]
            held, m = self.levels[above], SIZES[above]
            held[m - 1] = total
            self.wires[above].send(0, lambda peer: held.at[m - 1], held)
            return
        width = D // NY
        mine = lax.broadcasted_iota(jnp.int32, (8, D), 0) == self.me["x"]
        row = jnp.sum(jnp.where(mine, total, 0.0), axis=0, keepdims=True)
        self.out[...] = functools.reduce(
            jnp.add,
            [jnp.where(self.me["y"] == k, row[:, k * width : (k + 1) * width], 0.0) for k in range(NY)],
        )

    def drain(self):
        for wire in self.wires.values():
            wire.drain()


COST = {"plane": 0.15, "blocks": 0.25, "middle": 1.05, "last": 0.3, "early": 0.52, "late": 1.3}
COST |= {"bplane": 0.15, "bblocks": 0.25}
BUSY = 11.3 / UNITS
WAY = {"exch": 4.5, "z": 4.3, "ret": 3.5}
GAIN = (("gain", 4.8), ("gain_z", 4.0), ("gain_x", 4.0), ("gain_y", 2.0), ("gain_dp", 0.0))
MARGIN = 2.0


def plan():
    units = lambda turn: range(turn * NR, (turn + 1) * NR)
    batches = [(turn, b) for turn in range(2) for b in range(BATCHES)]
    needs, rank = {}, {}
    for u in range(UNITS):
        needs["plane", u] = [("exch", u)]
        needs["blocks", u] = [("z", u)]
        needs["bplane", u] = [("bexch", u)]
        needs["bblocks", u] = [("bz", u)]
    for turn, b in batches:
        key = turn * BATCHES + b
        needs["early", key] = []
        needs["middle", key] = [("ret", u) for u in units(turn)] + [("early", key)]
        needs["late", key] = [("middle", key)]
        needs["last", key] = [("bret", u) for u in units(turn)] + [("late", key)]
    before = None
    for name, _ in GAIN:
        needs[name, 0] = [before] if before else [("middle", n) for n in range(2 * BATCHES)]
        before = (name, 0)
    order_of = ["plane", "blocks", "bplane", "bblocks", "middle", "last"]
    links = {"plane": 0.0, "z": 0.0}
    done = {}
    now = 0.0

    def send(what, link, share, way):
        links[link] = max(now, links[link]) + BUSY * share
        done[what] = links[link] + way

    for u in range(UNITS):
        send(("exch", u), "plane", 1, WAY["exch"])
    order, left = [], dict(needs)
    while left:
        at = {k: max([done.get(d, 1e9) for d in v], default=0.0) for k, v in left.items()}
        fits = [
            (order_of.index(k[0]), k[1], k) for k in left if k[0] in order_of and at[k] <= now
        ]
        sums = [k for k in left if k[0].startswith("gain") and at[k] <= now]
        known = [at[k] for k in left if now < at[k] < 1e8]
        soon = min([at[k] for k in left if k[0] in order_of and now < at[k] < 1e8], default=1e9)
        if not fits:
            for k in left:
                if k[0] in ("middle", "last"):
                    filler = ("early" if k[0] == "middle" else "late", k[1])
                    rest = [d for d in needs[k] if d != filler]
                    if filler in left and at[filler] <= now and all(done.get(d, 1e9) <= now for d in rest):
                        fits.append((9, k[1], filler))
        if fits:
            pick = min(fits)[2]
        elif sums:
            pick = sums[0]
        else:
            spare = [
                (k[0] == "late", k[1], k)
                for k in left
                if k[0] in ("early", "late") and at[k] <= now and (now + COST[k[0]] <= soon + 0.15 or soon >= 1e8)
            ]
            if not spare:
                now = min(known)
                continue
            pick = min(spare)[2]
        name, key = pick
        order.append(pick)
        del left[pick]
        now += COST.get(name, 0.1)
        done[pick] = now
        if name.startswith("gain"):
            done[pick] = now + dict(GAIN)[name] + MARGIN
        if name in ("plane", "bplane"):
            send(("z" if name == "plane" else "bz", key), "z", 1, WAY["z"])
        if name in ("blocks", "bblocks"):
            send(("ret" if name == "blocks" else "bret", key), "plane", 1, WAY["ret"])
        if name == "middle":
            turn, b = divmod(key, BATCHES)
            first, *others = units(turn)
            send(("bexch", first), "plane", 1 / BATCHES, WAY["exch"])
            if b < BATCHES - 1:
                done.pop(("bexch", first))
            else:
                for u in others:
                    send(("bexch", u), "plane", 1, WAY["exch"])
    return order, now


def cols(head):
    return pl.ds(pl.multiple_of(head * D, D), D)


def mm(a, b, da, db):
    return lax.dot_general(a, b, (((da,), (db,)), ((), ())), preferred_element_type=F32)


def kernel(*refs):
    sources, (out, gq, gk, gv, gain_sum), refs = refs[:6], refs[6:11], refs[11:]
    (q, k, v, g_out, log_decay, gain, in_sems), refs = refs[:7], refs[7:]
    nd, ns = len(Decays.scratch), len(Scan.scratch)
    total, cum, cums, inside, wts, weights, ga, gkp, gvp, gain_part, local, prior, later_local, later = refs[:14]
    refs = refs[14:]
    me = here()
    decays = Decays(me, refs[:nd], total)
    refs = refs[nd:]
    fore = Scan(me, refs[:ns], decays, local, prior, False)
    back = Scan(me, refs[ns : 2 * ns], decays, later_local, later, True)
    sums = Gain(me, refs[2 * ns :], gain_part, gain_sum)

    met = greet(me)
    held = (q, k, v, g_out, log_decay, gain)
    loads = [pltpu.make_async_copy(a, b, in_sems.at[n]) for n, (a, b) in enumerate(zip(sources, held))]
    for n in (4, 1, 2, 0, 3, 5):
        loads[n].start()
    loads[4].wait()
    upper = (
        lax.broadcasted_iota(jnp.int32, (T, T), 0) <= lax.broadcasted_iota(jnp.int32, (T, T), 1)
    ).astype(F32)
    running = lax.dot_general(
        log_decay[...], upper, (((1,), (0,)), ((), ())), precision=lax.Precision.HIGHEST, preferred_element_type=F32
    )
    cum[...] = running
    gain_part[...] = jnp.zeros_like(gain_part)
    total[...] = jnp.zeros_like(total)
    blocks = jnp.broadcast_to(running[:, T - 1 : T], (HEADS, D))
    for o in range(NP):
        total[o, 0:2, :] = blocks[2 * o : 2 * o + 2]

    def for_heads(turn, work, begin=0, end=NP, at_once=4):
        at_once = min(at_once, end - begin)

        def step(n, carry):
            for u in range(at_once):
                s = begin + n * at_once + u + 1
                x = lax.rem(me["x"] + s // NY, NX)
                y = lax.rem(me["y"] + s % NY, NY)
                owner = x * NY + y
                work(owner, 2 * owner + turn)
            return carry

        if end - begin == at_once:
            step(0, 0)
        else:
            lax.fori_loop(0, (end - begin) // at_once, step, 0)

    def batch(key):
        turn, b = divmod(key, BATCHES)
        return turn, b * PER, (b + 1) * PER

    def weight(head):
        by_row = cums[head]
        gap = jnp.concatenate([by_row, by_row[:, : T - D]], axis=1) - cum[pl.ds(head, 1), :]
        causal = lax.broadcasted_iota(jnp.int32, (T, T), 0) >= lax.broadcasted_iota(jnp.int32, (T, T), 1)
        return jnp.exp(jnp.where(causal, gap, -1e30))

    def end_scale(head):
        by_row = cums[head]
        return jnp.exp(by_row[T - 1 : T, :] - by_row)

    def local_of(turn):
        def work(owner, head):
            by_row = jnp.transpose(jnp.broadcast_to(cum[pl.ds(head, 1), :], (D, T)))
            cums[head] = by_row
            scale = jnp.exp(by_row[T - 1 : T, :] - by_row)
            decayed = (k[:, cols(head)].astype(F32) * scale).astype(BF)
            local[owner, turn] = mm(decayed, v[:, cols(head)], 0, 0).astype(BF)

        for_heads(turn, work)

    def early(key):
        turn, begin, end = batch(key)

        def work(owner, head):
            scores = mm(q[:, cols(head)], k[:, cols(head)], 1, 1)
            factor = weight(head)
            weights[head] = factor
            weighted = (scores * factor).astype(BF)
            wts[head] = weighted
            inside[head] = mm(weighted, v[:, cols(head)], 1, 0)

        for_heads(turn, work, begin, end)

    def middle(key):
        turn, begin, end = batch(key)
        if begin == 0:
            fore.arrive(turn)

        def work(owner, head):
            state = fore.state(turn, owner)
            start = jnp.exp(cums[head])
            qh = q[:, cols(head)]
            attended = inside[head] + mm(qh, state, 1, 0) * start
            inv = lax.rsqrt(jnp.mean(attended * attended, axis=1, keepdims=True) + epsilon)
            normed = attended * inv
            row = gain[pl.ds(head, 1), :]
            out[:, cols(head)] = (normed * row).astype(BF)
            grad = g_out[:, cols(head)].astype(F32)
            scaled = grad * row
            lean = jnp.mean(scaled * normed, axis=1, keepdims=True)
            attended_grad = (inv * (scaled - normed * lean)).astype(BF)
            ga[head] = attended_grad
            gain_part[head // 4, pl.ds(lax.rem(head, 4), 1), :] = jnp.sum(grad * normed, axis=0, keepdims=True)
            decayed = (qh.astype(F32) * start).astype(BF)
            later_local[owner, turn] = mm(decayed, attended_grad, 0, 0).astype(BF)

        for_heads(turn, work, begin, end)
        back.start(turn * NR, range(begin + 1, end + 1))
        if end == NP:
            for r in range(1, NR):
                back.start(turn * NR + r, range(1, NP + 1))

    def late(key):
        turn, begin, end = batch(key)

        def work(owner, head):
            grad = ga[head]
            grad_scores = mm(grad, v[:, cols(head)], 1, 1)
            gw = (grad_scores * weights[head]).astype(BF)
            state = fore.state(turn, owner)
            gq[:, cols(head)] = (mm(gw, k[:, cols(head)], 1, 0) + jnp.exp(cums[head]) * mm(grad, state, 1, 1)).astype(BF)
            gkp[head] = mm(gw, q[:, cols(head)], 0, 0)
            gvp[head] = mm(wts[head], grad, 0, 0)

        for_heads(turn, work, begin, end)

    def last(key):
        turn, begin, end = batch(key)
        if begin == 0:
            back.arrive(turn)

        def work(owner, head):
            state = back.state(turn, owner)
            scale = end_scale(head)
            gk[:, cols(head)] = (gkp[head] + scale * mm(v[:, cols(head)], state, 1, 1)).astype(BF)
            gv[:, cols(head)] = (gvp[head] + scale * mm(k[:, cols(head)], state, 1, 0)).astype(BF)

        for_heads(turn, work, begin, end)

    stages = {
        "early": early,
        "plane": fore.over_plane,
        "blocks": fore.before_blocks,
        "middle": middle,
        "late": late,
        "bplane": back.over_plane,
        "bblocks": back.before_blocks,
        "last": last,
        "gain": lambda key: sums.start(),
    }
    for axis in sums.AXES:
        stages[f"gain_{axis}"] = lambda key, axis=axis: sums.fold(axis)
    loads[1].wait()
    loads[2].wait()
    local_of(0)
    met()
    decays.start()
    for u in range(NR):
        fore.start(u, range(1, NP + 1))
    local_of(1)
    for u in range(NR, UNITS):
        fore.start(u, range(1, NP + 1))
    first = {"early": lambda: loads[0].wait(), "plane": decays.lift, "blocks": decays.settle}
    first["middle"] = lambda: (loads[3].wait(), loads[5].wait())
    first["gain"] = lambda: (fore.drain(), decays.drain())
    for name, g in plan()[0]:
        first.pop(name, lambda: None)()
        stages[name](g)
    back.drain()
    sums.drain()


PARTS = 4


def store_kernel(*refs):
    given, kept, sems = refs[:5], refs[5:10], refs[10]
    copies = [pltpu.make_async_copy(given[4], kept[4], sems.at[4 * PARTS])]
    for n in range(4):
        for p in range(PARTS):
            rows = pl.ds(p * (T // PARTS), T // PARTS)
            copies.append(pltpu.make_async_copy(given[n].at[rows], kept[n].at[rows], sems.at[n * PARTS + p]))
    for copy in copies:
        copy.start()
    for copy in copies:
        copy.wait()


def body(queries, key_vectors, value_vectors, out_grad, log_decay, norm_gain):
    shape = queries.shape
    rows = (T, shape[-1])
    last_row = (1, D // NY)
    vmem = pl.BlockSpec(memory_space=pltpu.VMEM)
    hbm = pl.BlockSpec(memory_space=pltpu.HBM)
    scratch = [
        pltpu.VMEM((NP, 8, D), F32),
        pltpu.VMEM((HEADS, T), F32),
        pltpu.VMEM((HEADS, T, D), F32),
        pltpu.VMEM((HEADS, T, D), F32),
        pltpu.VMEM((HEADS, T, T), BF),
        pltpu.VMEM((HEADS, T, T), F32),
        pltpu.VMEM((HEADS, T, D), BF),
        pltpu.VMEM((HEADS, T, D), F32),
        pltpu.VMEM((HEADS, T, D), F32),
        pltpu.VMEM((NZ, 8, D), F32),
        pltpu.VMEM((NP, 2, D, D), BF),
        pltpu.VMEM((UNITS, NP, RR, D), BF),
        pltpu.VMEM((NP, 2, D, D), BF),
        pltpu.VMEM((UNITS, NP, RR, D), BF),
    ]
    results = pl.pallas_call(
        kernel,
        out_shape=[pltpu.VMEM(rows, BF)] * 4 + [pltpu.VMEM(last_row, F32)],
        in_specs=[hbm] * 6,
        out_specs=[vmem] * 5,
        scratch_shapes=[
            *[pltpu.VMEM(rows, BF)] * 4,
            pltpu.VMEM((HEADS, T), F32),
            pltpu.VMEM((HEADS, D), F32),
            pltpu.SemaphoreType.DMA((6,)),
            *scratch,
            *Decays.scratch,
            *Scan.scratch,
            *Scan.scratch,
            *Gain.scratch,
        ],
        compiler_params=pltpu.CompilerParams(
            collective_id=0, has_side_effects=True, vmem_limit_bytes=48 * 1024 * 1024
        ),
        name="attention",
    )(
        *[a.reshape(rows) for a in (queries, key_vectors, value_vectors, out_grad)],
        log_decay.reshape(HEADS, T),
        norm_gain.reshape(HEADS, D),
    )
    results = pl.pallas_call(
        store_kernel,
        out_shape=[jax.ShapeDtypeStruct(rows, BF)] * 4 + [jax.ShapeDtypeStruct(last_row, F32)],
        in_specs=[vmem] * 5,
        out_specs=[hbm] * 5,
        scratch_shapes=[pltpu.SemaphoreType.DMA((4 * PARTS + 1,))],
        compiler_params=pltpu.CompilerParams(vmem_limit_bytes=1024 * 1024),
        name="store",
    )(*results)
    return (*[r.reshape(shape) for r in results[:4]], results[4].reshape(D // NY))


def solution(mesh):
    split = Mesh(mesh.devices.reshape(NZ, NX, NY, mesh.shape["dp"]), AXES)
    rows = P("dp", SEQ, None)
    return jax.shard_map(
        body,
        mesh=split,
        in_specs=(rows, rows, rows, rows, P("dp", None, SEQ), P()),
        out_specs=(rows, rows, rows, rows, P(SEQ)),
        check_vma=False,
    )
```
